32 devices in a mesh: ctx: 8 (over y, x, core), head: 4 (over z).
Axes of the slice: x: 2, y: 2, z: 4, core: 2. Of those that a mesh axis runs over, the one named last changes fastest.
Arguments:
- tokens: bfloat16 [4096, 5376], P('ctx'), may hold values from -16 to 16
- norm_gain: bfloat16 [5376], replicated, may hold values from 0.099609375 to 1.8984375
- w_query: bfloat16 [5376, 4096], P(None, 'head'), may hold values from -4 to 4
- w_key: bfloat16 [5376, 2048], P(None, 'head'), may hold values from -1 to 1
- value_weight: bfloat16 [5376, 2048], P(None, 'head'), may hold values from -0.078125 to 0.078125
- w_out: bfloat16 [4096, 5376], P('head'), may hold values from -0.09375 to 0.09375
- mask_logit: float32 [32], P('head'), may hold values from -2 to 2
- noise_draw: float32 [32], P('head'), may hold values from 0.02 to 0.98
- cotangent: bfloat16 [4096, 5376], P('ctx'), may hold values from -16 to 16
Outputs:
- layer_out: bfloat16 [4096, 5376], P('ctx', 'head')
- grad_logit: float32 [32], P('head')
- grad_out_proj: float32 [4096, 5376], P('head', 'ctx')
The draws below stay inside these ranges and needn't reach their ends.
All inputs are finite; a program needn't handle non-finite values.
Results may differ from the reference program's by a relative error of at most 0.025.
Values may be sent and summed in bfloat16 or wider, within the bound.
No kernel may reach another device: no remote copies, remote signals or barrier semaphores. Data moves between devices by JAX's collectives and lax.ppermute only.
A program may use at most 128 MiB of HBM per device.

```python
import math
import jax
import jax.numpy as jnp
from jax import lax

MODEL_WIDTH = 5376
QUERY_HEADS = 32
KEY_VALUE_HEADS = 16
HEAD_SIZE = 128
WINDOW_TOKENS = 1024
TOKENS = 4096
N_HEAD = 4


def draw_tokens(key, part):
    normal_rows = jax.random.normal(jax.random.fold_in(key, 11), (TOKENS, MODEL_WIDTH), jnp.float32)
    values = normal_rows
    return jnp.clip(values, -16.0, 16.0).astype(jnp.bfloat16)


def projection_pair(key):
    key_portion = jax.random.normal(jax.random.fold_in(key, 21), (MODEL_WIDTH, KEY_VALUE_HEADS * HEAD_SIZE), jnp.float32) / math.sqrt(MODEL_WIDTH)
    extra = jax.random.normal(jax.random.fold_in(key, 22), (MODEL_WIDTH, QUERY_HEADS * HEAD_SIZE), jnp.float32) / math.sqrt(MODEL_WIDTH)
    query_part = 2.3 * extra
    return (jnp.clip(query_part, -4.0, 4.0), jnp.clip(key_portion, -1.0, 1.0))


def draw_w_query(key, part):
    return projection_pair(key)[0].astype(jnp.bfloat16)


def draw_w_key(key, part):
    return projection_pair(key)[1].astype(jnp.bfloat16)


def draw_cotangent(key, part):
    position = jnp.arange(TOKENS, dtype=jnp.float32) / max(TOKENS - 1, 1)
    rising = (3.0 ** position)[:, None]
    values = rising * jax.random.normal(jax.random.fold_in(key, 33), (TOKENS, MODEL_WIDTH), jnp.float32)
    return jnp.clip(values, -16.0, 16.0).astype(jnp.bfloat16)


def steps_of(key, dims, cuts, low, high):
    def one(dim, shards_of):
        heights = jax.random.uniform(jax.random.fold_in(jax.random.fold_in(key, 6), dim), (shards_of,), jnp.float32, low / len(cuts), high / len(cuts))
        return jnp.repeat(jnp.exp(heights), dims[dim] // shards_of).reshape((-1,) + (1,) * (len(dims) - dim - 1))

    factor_of = one(*cuts[0])
    for cut in cuts[1:]:
        factor_of = factor_of * one(*cut)
    return factor_of


def bell_draw(own_key, extent, scale, reach, pieces=(), kind=jnp.bfloat16):
    entries = scale * jax.random.normal(own_key, extent, jnp.float32)
    if pieces:
        entries = entries * steps_of(own_key, extent, pieces, -0.22, 0.18)
    return jnp.clip(entries, -reach, reach).astype(kind)


def setup_inputs(seed: int = 0) -> dict:
    key_of = jax.random.split(jax.random.key(seed), 10)
    tokens = draw_tokens(jax.random.fold_in(key_of[9], 71), 0)
    norm_gain = jnp.clip(1.0 + 0.18 * jax.random.normal(key_of[1], (MODEL_WIDTH,), jnp.float32), 0.099609375, 1.8984375).astype(jnp.bfloat16)
    w_query = draw_w_query(jax.random.fold_in(key_of[9], 71), 0)
    w_key = draw_w_key(jax.random.fold_in(key_of[9], 71), 0)
    value_weight = bell_draw(key_of[4], (MODEL_WIDTH, KEY_VALUE_HEADS * HEAD_SIZE), MODEL_WIDTH ** -0.5, 0.078125, ((1, 4),))
    w_out = bell_draw(key_of[5], (QUERY_HEADS * HEAD_SIZE, MODEL_WIDTH), (QUERY_HEADS * HEAD_SIZE) ** -0.5, 0.09375, ((0, 4),))
    mask_logit = jnp.clip(jax.random.uniform(key_of[6], (QUERY_HEADS,), jnp.float32, -2.0, 2.0) * steps_of(key_of[6], (QUERY_HEADS,), ((0, 4),), -0.4, 0.0), -2.0, 2.0)
    noise_draw = jnp.clip(0.02 + 0.96000002 * jax.random.uniform(key_of[7], (QUERY_HEADS,), jnp.float32) ** steps_of(key_of[7], (QUERY_HEADS,), ((0, 4),), -0.2, 0.2), 0.02, 0.98)
    cotangent = draw_cotangent(jax.random.fold_in(key_of[9], 71), 0)
    return dict(tokens=tokens, norm_gain=norm_gain, w_query=w_query, w_key=w_key, value_weight=value_weight, w_out=w_out, mask_logit=mask_logit, noise_draw=noise_draw, cotangent=cotangent)


EPSILON = 1e-06
BETA = 2.0 / 3.0
GAMMA = -0.1
ZETA = 1.1
PENALTY = 0.1
SCORE_SCALE = 168.0 ** (-0.5)
TRANSPOSED = (((0,), (0,)), ((), ()))

def hard_concrete(mask_logit, noise_draw):
    logit = mask_logit.astype(jnp.float32)
    uniform_value = noise_draw.astype(jnp.float32)
    stretched = jax.nn.sigmoid((jnp.log(uniform_value) - jnp.log(1.0 - uniform_value) + logit) / BETA)
    shifted = stretched * (ZETA - GAMMA) + GAMMA
    gate_value = jnp.clip(shifted, 0.0, 1.0)
    inside = jnp.logical_and(shifted > 0.0, shifted < 1.0)
    gate_slope = jnp.where(inside, (ZETA - GAMMA) * stretched * (1.0 - stretched) / BETA, 0.0)
    expected = jax.nn.sigmoid(logit - BETA * math.log(-GAMMA / ZETA))
    return (gate_value, gate_slope, PENALTY * expected * (1.0 - expected))

def attend(query_rows, rows_of_keys, rows_of_values):
    every_row = query_rows.shape[0]
    rows_per_block = math.gcd(every_row, 512)
    group_count_heads = QUERY_HEADS // KEY_VALUE_HEADS
    blocks_of_queries = query_rows.reshape(every_row // rows_per_block, rows_per_block, KEY_VALUE_HEADS, group_count_heads, HEAD_SIZE)
    pad_amount = jnp.zeros((WINDOW_TOKENS, KEY_VALUE_HEADS * HEAD_SIZE), rows_of_keys.dtype)
    padded_keys = jnp.concatenate([pad_amount, rows_of_keys], axis=0).reshape(WINDOW_TOKENS + every_row, KEY_VALUE_HEADS, HEAD_SIZE)
    padded_values = jnp.concatenate([pad_amount, rows_of_values], axis=0).reshape(WINDOW_TOKENS + every_row, KEY_VALUE_HEADS, HEAD_SIZE)

    def one_block(block_index):
        first_row = block_index * rows_per_block
        query_block = lax.dynamic_index_in_dim(blocks_of_queries, block_index, 0, keepdims=False)
        key_block = lax.dynamic_slice_in_dim(padded_keys, first_row, WINDOW_TOKENS + rows_per_block, 0)
        value_block = lax.dynamic_slice_in_dim(padded_values, first_row, WINDOW_TOKENS + rows_per_block, 0)
        scores = jnp.einsum('rkgd,lkd->kgrl', query_block.astype(jnp.float32), key_block.astype(jnp.float32)) * SCORE_SCALE
        query_pos = first_row + jnp.arange(rows_per_block, dtype=jnp.int32)[:, None]
        key_pos = first_row - WINDOW_TOKENS + jnp.arange(WINDOW_TOKENS + rows_per_block, dtype=jnp.int32)[None, :]
        allowed = (key_pos <= query_pos) & (query_pos - key_pos < WINDOW_TOKENS) & (key_pos >= 0)
        scores = jnp.where(allowed, scores, -jnp.inf)
        row_max = lax.optimization_barrier(jnp.max(scores, axis=-1, keepdims=True))
        lifted = jnp.exp(scores - row_max)
        prob_rows = (lifted / lax.optimization_barrier(jnp.sum(lifted, axis=-1, keepdims=True))).astype(jnp.bfloat16)
        attended = jnp.einsum('kgrl,lkd->rkgd', prob_rows.astype(jnp.float32), value_block.astype(jnp.float32))
        return attended.astype(jnp.bfloat16).reshape(rows_per_block, QUERY_HEADS * HEAD_SIZE)
    blocks = lax.map(one_block, jnp.arange(every_row // rows_per_block, dtype=jnp.int32))
    return blocks.reshape(every_row, QUERY_HEADS * HEAD_SIZE)

def reference(tokens, norm_gain, w_query, w_key, value_weight, w_out, mask_logit, noise_draw, cotangent):
    widened = tokens.astype(jnp.float32)
    moment = lax.optimization_barrier(jnp.mean(jnp.square(widened), axis=1, keepdims=True))
    normed = (widened * lax.rsqrt(moment + EPSILON) * norm_gain.astype(jnp.float32)[None, :]).astype(jnp.bfloat16)
    query_rows = jnp.dot(normed, w_query, preferred_element_type=jnp.float32).astype(jnp.bfloat16)
    rows_of_keys = jnp.dot(normed, w_key, preferred_element_type=jnp.float32).astype(jnp.bfloat16)
    rows_of_values = jnp.dot(normed, value_weight, preferred_element_type=jnp.float32).astype(jnp.bfloat16)
    attended = attend(query_rows, rows_of_keys, rows_of_values)
    gate_value, gate_slope, penalty_term = hard_concrete(mask_logit, noise_draw)
    gate_columns = jnp.repeat(gate_value, HEAD_SIZE)
    gated = (attended.astype(jnp.float32) * gate_columns[None, :]).astype(jnp.bfloat16)
    group_width = QUERY_HEADS * HEAD_SIZE // N_HEAD
    gated_groups = gated.reshape(TOKENS, N_HEAD, group_width)
    weight_groups = w_out.reshape(N_HEAD, group_width, MODEL_WIDTH)

    def add_group(running, group_index):
        piece_in = lax.dynamic_index_in_dim(gated_groups, group_index, 1, keepdims=False)
        piece_weight = lax.dynamic_index_in_dim(weight_groups, group_index, 0, keepdims=False)
        partial_out = jnp.dot(piece_in, piece_weight, preferred_element_type=jnp.float32).astype(jnp.bfloat16)
        partial_out = lax.optimization_barrier(partial_out)
        return (running + partial_out.astype(jnp.float32), None)
    summed_out, unused = lax.scan(add_group, jnp.zeros((TOKENS, MODEL_WIDTH), jnp.float32), jnp.arange(N_HEAD, dtype=jnp.int32))
    layer_out = summed_out.astype(jnp.bfloat16)
    inv_root = 1.0 / math.sqrt(TOKENS)
    through = lax.dot_general(cotangent, w_out, (((1,), (1,)), ((), ())), preferred_element_type=jnp.float32)
    gate_product = lax.optimization_barrier(jnp.sum((through * attended.astype(jnp.float32)).reshape(TOKENS, QUERY_HEADS, HEAD_SIZE), axis=(0, 2))) * inv_root
    grad_logit = gate_product * gate_slope + penalty_term
    weight_sum = lax.dot_general(attended, cotangent, TRANSPOSED, preferred_element_type=jnp.float32)
    grad_out_proj = weight_sum * gate_columns[:, None] * inv_root
    return (layer_out, grad_logit, grad_out_proj)
```

```python
import functools
import math

import jax
import jax.numpy as jnp
from jax import lax
from jax.experimental import pallas as pl
from jax.experimental.pallas import tpu as pltpu
from jax.sharding import PartitionSpec as P


HEAD_SIZE = 128
WINDOW_TOKENS = 1024

EPSILON = 1e-06
BETA = 2.0 / 3.0
GAMMA = -0.1
ZETA = 1.1
PENALTY = 0.1
SCORE_SCALE = 168.0 ** (-0.5)
LOG2_E = 1.4426950408889634


def shift(value, axis, steps):
    count = lax.axis_size(axis)
    return lax.ppermute(value, axis, [(i, i + steps) for i in range(count - steps)])


def rotate(value, axis, steps):
    count = lax.axis_size(axis)
    return lax.ppermute(value, axis, [(i, (i + steps) % count) for i in range(count)])


def swap(value, axis, bit):
    count = lax.axis_size(axis)
    return lax.ppermute(value, axis, [(i, i ^ bit) for i in range(count)])


def hard_concrete(mask_logit, noise_draw):
    stretched = jax.nn.sigmoid(
        (jnp.log(noise_draw) - jnp.log(1.0 - noise_draw) + mask_logit) / BETA
    )
    shifted = stretched * (ZETA - GAMMA) + GAMMA
    gate_value = jnp.clip(shifted, 0.0, 1.0)
    inside = jnp.logical_and(shifted > 0.0, shifted < 1.0)
    gate_slope = jnp.where(inside, (ZETA - GAMMA) * stretched * (1.0 - stretched) / BETA, 0.0)
    expected = jax.nn.sigmoid(mask_logit - BETA * math.log(-GAMMA / ZETA))
    return (gate_value, gate_slope, PENALTY * expected * (1.0 - expected))


def after(value, *others):
    return lax.optimization_barrier((value,) + others)[0]


def attention_kernel(pos_ref, q_ref, k2_ref, k1_ref, k0_ref, v2_ref, v1_ref, v0_ref, gate_ref,
                     att_ref, gated_ref, *, block, group):
    rows = q_ref.shape[0]
    position = pos_ref[0]
    keys = (k2_ref, k1_ref, k0_ref)
    values = (v2_ref, v1_ref, v0_ref)
    bias = (
        jnp.where(position >= 2, 0.0, -jnp.inf).astype(jnp.float32),
        jnp.where(position >= 1, 0.0, -jnp.inf).astype(jnp.float32),
        None,
    )
    per = rows // block
    count = WINDOW_TOKENS // block + 1
    ones = jnp.ones((block, HEAD_SIZE), jnp.bfloat16)
    row_id = lax.broadcasted_iota(jnp.int32, (block, block), 0)
    col_id = lax.broadcasted_iota(jnp.int32, (block, block), 1)
    behind = jnp.concatenate([col_id > row_id] * group, axis=0)
    ahead = jnp.concatenate([col_id <= row_id] * group, axis=0)
    for b in range(per):
        here = pl.ds(b * block, block)
        query = jnp.concatenate(
            [q_ref[here, g * HEAD_SIZE:(g + 1) * HEAD_SIZE] for g in range(group)], axis=0
        )
        scores = []
        for s in range(count):
            piece, offset = divmod(b + s, per)
            key = keys[piece][pl.ds(offset * block, block), :]
            score = lax.dot_general(
                query, key, (((1,), (1,)), ((), ())), preferred_element_type=jnp.float32
            )
            if s == 0:
                score = jnp.where(behind, score, -jnp.inf)
            if s == count - 1:
                score = jnp.where(ahead, score, -jnp.inf)
            if bias[piece] is not None:
                score = score + bias[piece]
            scores.append(score)
        top = functools.reduce(jnp.maximum, scores)
        top = jnp.max(top, axis=1, keepdims=True)
        total = None
        for s in range(count):
            piece, offset = divmod(b + s, per)
            prob = jnp.exp2((scores[s] - top) * (SCORE_SCALE * LOG2_E)).astype(jnp.bfloat16)
            value = jnp.concatenate(
                [values[piece][pl.ds(offset * block, block), :], ones], axis=1
            )
            part = jnp.dot(prob, value, preferred_element_type=jnp.float32)
            total = part if total is None else total + part
        result = (total[:, :HEAD_SIZE] / total[:, HEAD_SIZE:]).astype(jnp.bfloat16)
        for g in range(group):
            cols = slice(g * HEAD_SIZE, (g + 1) * HEAD_SIZE)
            piece_out = result[g * block:(g + 1) * block]
            att_ref[here, cols] = piece_out
            gated_ref[here, cols] = (
                piece_out.astype(jnp.float32) * gate_ref[:, cols]
            ).astype(jnp.bfloat16)


def attention(position, queries, kv2, kv1, kv0, gate_row, side):
    rows = queries.shape[0]
    kv_heads = kv0.shape[1] // (2 * HEAD_SIZE)
    wide = queries.shape[1] // (2 * kv_heads)
    group = wide // HEAD_SIZE
    width = kv_heads * wide
    block = math.gcd(rows, 256)
    key_spec = pl.BlockSpec((rows, HEAD_SIZE), lambda h, pos: (0, h))
    value_spec = pl.BlockSpec((rows, HEAD_SIZE), lambda h, pos: (0, kv_heads + h))
    query_spec = pl.BlockSpec((rows, wide), lambda h, pos: (0, side * kv_heads + h))
    out_spec = pl.BlockSpec((rows, wide), lambda h, pos: (0, h))
    return pl.pallas_call(
        functools.partial(attention_kernel, block=block, group=group),
        grid_spec=pltpu.PrefetchScalarGridSpec(
            num_scalar_prefetch=1,
            grid=(kv_heads,),
            in_specs=[query_spec, key_spec, key_spec, key_spec, value_spec, value_spec, value_spec,
                      pl.BlockSpec((1, wide), lambda h, pos: (0, side * kv_heads + h))],
            out_specs=[out_spec, out_spec],
        ),
        out_shape=[jax.ShapeDtypeStruct((rows, width), jnp.bfloat16)] * 2,
        compiler_params=pltpu.CompilerParams(dimension_semantics=("arbitrary",)),
        cost_estimate=pl.CostEstimate(
            flops=8 * rows * (WINDOW_TOKENS + block) * width, bytes_accessed=10 * rows * width,
            transcendentals=rows * (WINDOW_TOKENS + block) * width // HEAD_SIZE),
        name="attention",
    )(position, queries, kv2, kv1, kv0, kv2, kv1, kv0, gate_row)


def terms_kernel(tab_ref, cot0_ref, cot1_ref, att0_ref, att1_ref, sent_ref, kept_ref, *, sent):
    index = pl.program_id(0)
    total = (
        jnp.dot(cot0_ref[0], att0_ref[...], preferred_element_type=jnp.float32)
        + jnp.dot(cot1_ref[0], att1_ref[...], preferred_element_type=jnp.float32)
    ).astype(jnp.bfloat16)

    @pl.when(index < sent)
    def _():
        sent_ref[0] = total

    @pl.when(index >= sent)
    def _():
        kept_ref[0] = total


def grad_terms(position, cot_blocks, cot_other, att, att_other, order):
    _, width, rows = cot_blocks.shape
    cols = att.shape[1]
    steps = len(order)
    sent = steps // 2
    owners = position ^ jnp.array(order, jnp.int32)
    table = jnp.concatenate([owners, owners // 2])
    whole = pl.BlockSpec((rows, cols), lambda j, tab: (0, 0))
    return pl.pallas_call(
        functools.partial(terms_kernel, sent=sent),
        grid_spec=pltpu.PrefetchScalarGridSpec(
            num_scalar_prefetch=1,
            grid=(steps,),
            in_specs=[
                pl.BlockSpec((1, width, rows), lambda j, tab: (tab[j], 0, 0)),
                pl.BlockSpec((1, width, rows), lambda j, tab: (tab[steps + j], 0, 0)),
                whole,
                whole,
            ],
            out_specs=[
                pl.BlockSpec((1, width, cols), lambda j, tab: (jnp.minimum(j, sent - 1), 0, 0)),
                pl.BlockSpec((1, width, cols), lambda j, tab: (jnp.maximum(j - sent, 0), 0, 0)),
            ],
        ),
        out_shape=[jax.ShapeDtypeStruct((sent, width, cols), jnp.bfloat16)] * 2,
        compiler_params=pltpu.CompilerParams(dimension_semantics=("arbitrary",)),
        cost_estimate=pl.CostEstimate(
            flops=4 * steps * width * rows * cols,
            bytes_accessed=2 * steps * width * (2 * rows + cols), transcendentals=0),
        name="grad_terms",
    )(table, cot_blocks, cot_other, att, att_other)


def project_kernel(pos_ref, *refs, turns, slots, count):
    pairs = 2 * len(turns)
    x_refs = refs[:pairs]
    rest = list(refs[pairs:])
    base_ref = rest.pop(0) if turns[0] != -1 else None
    own_ref = rest.pop(0) if turns[0] == -1 else None
    w_refs = rest[:len(slots)]
    out_ref, weight, sems = rest[len(slots):]
    position = pos_ref[0]
    copies = []
    for k, turn in enumerate(turns):
        group = []
        if turn == -1:
            group.append(pltpu.make_async_copy(own_ref, weight.at[k], sems.at[k, 0]))
        else:
            for index, relative in enumerate(slots):
                start = pl.multiple_of((position ^ relative) * count, count)
                group.append(pltpu.make_async_copy(
                    w_refs[index].at[pl.ds(turn * count, count)], weight.at[k, pl.ds(start, count)], sems.at[k, index]))
        for copy in group:
            copy.start()
        copies.append(group)
    total = None if base_ref is None else base_ref[...]
    middle = x_refs[0].shape[1]
    for k in range(len(turns)):
        for copy in copies[k]:
            copy.wait()
        for side in range(2):
            part = jnp.dot(
                x_refs[2 * k + side][...],
                weight[k, side * middle:(side + 1) * middle],
                preferred_element_type=jnp.float32,
            )
            total = part if total is None else total + part
    out_ref[...] = total[:, :out_ref.shape[1]].astype(out_ref.dtype)


def project(position, xs, base, own, weights, slots, turns, out_cols, dtype):
    rows, middle = xs[0].shape
    cols = weights[0].shape[1]
    whole = pl.BlockSpec(memory_space=pltpu.VMEM)
    anywhere = pl.BlockSpec(memory_space=pl.ANY)
    extra = [own] if base is None else [base]
    return pl.pallas_call(
        functools.partial(project_kernel, turns=turns, slots=slots, count=2 * middle // len(slots)),
        in_specs=[pl.BlockSpec(memory_space=pltpu.SMEM)] + [whole] * len(xs)
        + [anywhere if base is None else whole] + [anywhere] * len(weights),
        out_specs=whole,
        out_shape=jax.ShapeDtypeStruct((rows, out_cols), dtype),
        scratch_shapes=[
            pltpu.VMEM((len(turns), 2 * middle, cols), jnp.bfloat16),
            pltpu.SemaphoreType.DMA((len(turns), len(slots))),
        ],
        cost_estimate=pl.CostEstimate(
            flops=4 * len(turns) * rows * middle * cols,
            bytes_accessed=len(turns) * 4 * middle * (rows + cols) + 8 * rows * cols,
            transcendentals=0),
        name="project",
    )(position, *xs, *extra, *weights)


def turned_kernel(x_ref, out_ref):
    out_ref[...] = x_ref[...].T


def turned(x):
    whole = pl.BlockSpec(memory_space=pltpu.VMEM)
    return pl.pallas_call(
        turned_kernel, in_specs=[whole], out_specs=whole,
        out_shape=jax.ShapeDtypeStruct(x.shape[::-1], x.dtype), name="turned",
    )(x)


def body(tokens, norm_gain, w_query, w_key, value_weight, w_out, mask_logit, noise_draw, cotangent):
    tok_rows, model_width = tokens.shape
    local_heads = mask_logit.shape[0]
    n_ctx = lax.axis_size("ctx")
    n_head = lax.axis_size("head")
    p = lax.axis_index("ctx")
    z = lax.axis_index("head")
    position = p.astype(jnp.int32).reshape(1)
    bits = [1 << k for k in range(1, n_ctx.bit_length() - 1)]
    inv_root = 1.0 / math.sqrt(tok_rows * n_ctx)
    out_cols = model_width // n_head
    wide_cols = -(-out_cols // 128) * 128
    piece = w_out.shape[0] // n_ctx

    mine = lax.dynamic_slice_in_dim(w_out, p * piece, piece, 0)
    turns = []
    for t in range(1, n_head):
        block = lax.dynamic_slice_in_dim(mine, ((z + t) % n_head) * out_cols, out_cols, 1)
        block = jnp.pad(block, ((0, 0), (0, wide_cols - out_cols)))
        turns.append(rotate(block, "head", t))

    widened = tokens.astype(jnp.float32)
    moment = jnp.mean(jnp.square(widened), axis=1, keepdims=True)
    normed = (
        widened * lax.rsqrt(moment + EPSILON) * norm_gain.astype(jnp.float32)[None, :]
    ).astype(jnp.bfloat16)
    keys = jnp.dot(normed, w_key, preferred_element_type=jnp.float32).astype(jnp.bfloat16)
    values = jnp.dot(normed, value_weight, preferred_element_type=jnp.float32).astype(
        jnp.bfloat16)
    kv_half = keys.shape[1] // 2
    kv_sides = []
    kv2_sides = []
    for h in range(2):
        cols = slice(h * kv_half, (h + 1) * kv_half)
        kv_sides.append(jnp.concatenate([keys[:, cols], values[:, cols]], axis=1))
        kv2_sides.append(shift(kv_sides[h], "ctx", 2))
    queries = jnp.dot(
        after(normed, *kv_sides), w_query, preferred_element_type=jnp.float32
    ).astype(jnp.bfloat16)

    gate_value, gate_slope, penalty_term = hard_concrete(mask_logit, noise_draw)
    gate_columns = jnp.repeat(gate_value, HEAD_SIZE)
    gate_row = gate_columns[None, :]

    own_part = jnp.concatenate(after(tuple(turns), queries), axis=0)
    parts = {0: own_part}
    for bit in bits:
        for relative in list(parts):
            parts[relative | bit] = swap(parts[relative], "ctx", bit)

    mixed = [jnp.where(p % 2 == 0, kv_sides[h], after(kv2_sides[h], queries)) for h in range(2)]

    cot_blocks = after(cotangent, mixed[0]).T.reshape(n_ctx, model_width // n_ctx, tok_rows)
    leaving = lax.dynamic_index_in_dim(
        cot_blocks.reshape((n_ctx // 2, 2) + cot_blocks.shape[1:]), 1 - p % 2, 1, keepdims=False)
    cot_other = swap(leaving, "ctx", 1)

    attended = []
    moving = []
    others = []
    for h in range(2):
        kv1 = swap(mixed[h], "ctx", 1)
        att, gat = attention(
            position, queries, kv2_sides[h], kv1, kv_sides[h], gate_row, h)
        attended.append(att)
        chain = [gat]
        for _ in range(1, n_head):
            chain.append(rotate(chain[-1], "head", 1))
        moving.append(chain)
        others.append(swap(att, "ctx", 1))

    own_weight = jnp.pad(
        lax.dynamic_slice_in_dim(after(w_out, attended[1]), z * out_cols, out_cols, 1),
        ((0, 0), (0, wide_cols - out_cols)))

    own_cols = model_width // n_ctx
    w_mine = lax.dynamic_slice_in_dim(after(w_out, attended[1]), p * own_cols, own_cols, 1)
    w_mine = turned(jnp.pad(w_mine, ((0, 0), (0, -own_cols % 128))))[:own_cols]

    grads = []
    for h in range(2):
        steps = bits if h == 0 else bits[::-1]
        relative = [2 * j for j in range(n_ctx // 2)]
        order = [r for r in relative if r & steps[0]] + [r for r in relative if not r & steps[0]]
        sent, kept = grad_terms(
            position, cot_blocks, cot_other, attended[h], others[h], order)
        relative = order[len(order) // 2:]
        for k, bit in enumerate(steps):
            if k:
                leave = [i for i, r in enumerate(relative) if r & bit]
                stay = [i for i, r in enumerate(relative) if not r & bit]
                sent = jnp.concatenate([total[i:i + 1] for i in leave], axis=0)
                kept = jnp.concatenate([total[i:i + 1] for i in stay], axis=0)
                relative = [relative[i] for i in stay]
            received = swap(sent, "ctx", bit)
            total = kept.astype(jnp.float32) + received.astype(jnp.float32)
            if len(relative) > 1:
                total = total.astype(jnp.bfloat16)
        grads.append(total[0])

    for relative in list(parts):
        parts[relative | 1] = swap(parts[relative], "ctx", 1)
    slots = tuple(parts)
    weights = [parts[r] for r in slots]

    early = list(range(n_head - 2))
    xs = [moving[h][0] for h in range(2)]
    for t in early:
        xs += [moving[h][t + 1] for h in range(2)]
    base = project(position, xs, None, own_weight, weights, slots, (-1,) + tuple(early),
                   wide_cols, jnp.float32)
    layer_out = project(position, [moving[h][-1] for h in range(2)], base, None, weights,
                        slots, (n_head - 2,), out_cols, jnp.bfloat16)

    summed = jnp.concatenate([g.T for g in grads], axis=0)
    grad_out_proj = summed * gate_columns[:, None] * inv_root

    head_terms = jnp.sum(
        (summed.T * w_mine.astype(jnp.float32)).reshape(-1, local_heads, HEAD_SIZE), axis=(0, 2))
    for bit in [1] + bits:
        head_terms = head_terms + swap(head_terms, "ctx", bit)
    grad_logit = head_terms * inv_root * gate_slope + penalty_term
    return (layer_out, grad_logit, grad_out_proj)


def solution(mesh):
    return jax.shard_map(
        body,
        mesh=mesh,
        in_specs=(
            P("ctx", None),
            P(),
            P(None, "head"),
            P(None, "head"),
            P(None, "head"),
            P("head", None),
            P("head"),
            P("head"),
            P("ctx", None),
        ),
        out_specs=(P("ctx", "head"), P("head"), P("head", "ctx")),
        check_vma=False,
    )
```

```python
import functools
import math

import jax
import jax.numpy as jnp
from jax import lax
from jax.experimental import pallas as pl
from jax.experimental.pallas import tpu as pltpu
from jax.sharding import PartitionSpec as P


HEAD_SIZE = 128
WINDOW_TOKENS = 1024

EPSILON = 1e-06
BETA = 2.0 / 3.0
GAMMA = -0.1
ZETA = 1.1
PENALTY = 0.1
SCORE_SCALE = 168.0 ** (-0.5)
LOG2_E = 1.4426950408889634


def shift(value, axis, steps):
    count = lax.axis_size(axis)
    return lax.ppermute(value, axis, [(i, i + steps) for i in range(count - steps)])


def rotate(value, axis, steps):
    count = lax.axis_size(axis)
    return lax.ppermute(value, axis, [(i, (i + steps) % count) for i in range(count)])


def swap(value, axis, bit):
    count = lax.axis_size(axis)
    return lax.ppermute(value, axis, [(i, i ^ bit) for i in range(count)])


def window_of(cols):
    step = math.gcd(cols, 128)
    return -(-(cols + 128 - step) // 128) * 128


def window_start(width, cols, index):
    first = index * cols // 128 * 128
    return jnp.minimum(first, width - window_of(cols))


def hard_concrete(mask_logit, noise_draw):
    stretched = jax.nn.sigmoid(
        (jnp.log(noise_draw) - jnp.log(1.0 - noise_draw) + mask_logit) / BETA
    )
    shifted = stretched * (ZETA - GAMMA) + GAMMA
    gate_value = jnp.clip(shifted, 0.0, 1.0)
    inside = jnp.logical_and(shifted > 0.0, shifted < 1.0)
    gate_slope = jnp.where(inside, (ZETA - GAMMA) * stretched * (1.0 - stretched) / BETA, 0.0)
    expected = jax.nn.sigmoid(mask_logit - BETA * math.log(-GAMMA / ZETA))
    return (gate_value, gate_slope, PENALTY * expected * (1.0 - expected))


def after(value, *others):
    return lax.optimization_barrier((value,) + others)[0]


def attention_kernel(pos_ref, q_ref, k2_ref, k1_ref, k0_ref, v2_ref, v1_ref, v0_ref, gate_ref,
                     att_ref, gated_ref, *, block, group):
    rows = q_ref.shape[0]
    position = pos_ref[0]
    keys = (k2_ref, k1_ref, k0_ref)
    values = (v2_ref, v1_ref, v0_ref)
    bias = (
        jnp.where(position >= 2, 0.0, -jnp.inf).astype(jnp.float32),
        jnp.where(position >= 1, 0.0, -jnp.inf).astype(jnp.float32),
        None,
    )
    per = rows // block
    count = WINDOW_TOKENS // block + 1
    ones = jnp.ones((block, HEAD_SIZE), jnp.bfloat16)
    row_id = lax.broadcasted_iota(jnp.int32, (block, block), 0)
    col_id = lax.broadcasted_iota(jnp.int32, (block, block), 1)
    behind = jnp.concatenate([col_id > row_id] * group, axis=0)
    ahead = jnp.concatenate([col_id <= row_id] * group, axis=0)
    for b in range(per):
        here = pl.ds(b * block, block)
        query = jnp.concatenate(
            [q_ref[here, g * HEAD_SIZE:(g + 1) * HEAD_SIZE] for g in range(group)], axis=0
        )
        scores = []
        for s in range(count):
            piece, offset = divmod(b + s, per)
            key = keys[piece][pl.ds(offset * block, block), :]
            score = lax.dot_general(
                query, key, (((1,), (1,)), ((), ())), preferred_element_type=jnp.float32
            )
            if s == 0:
                score = jnp.where(behind, score, -jnp.inf)
            if s == count - 1:
                score = jnp.where(ahead, score, -jnp.inf)
            if bias[piece] is not None:
                score = score + bias[piece]
            scores.append(score)
        top = functools.reduce(jnp.maximum, scores)
        top = jnp.max(top, axis=1, keepdims=True)
        total = None
        for s in range(count):
            piece, offset = divmod(b + s, per)
            prob = jnp.exp2((scores[s] - top) * (SCORE_SCALE * LOG2_E)).astype(jnp.bfloat16)
            value = jnp.concatenate(
                [values[piece][pl.ds(offset * block, block), :], ones], axis=1
            )
            part = jnp.dot(prob, value, preferred_element_type=jnp.float32)
            total = part if total is None else total + part
        result = (total[:, :HEAD_SIZE] / total[:, HEAD_SIZE:]).astype(jnp.bfloat16)
        for g in range(group):
            cols = slice(g * HEAD_SIZE, (g + 1) * HEAD_SIZE)
            piece_out = result[g * block:(g + 1) * block]
            att_ref[here, cols] = piece_out
            gated_ref[here, cols] = (
                piece_out.astype(jnp.float32) * gate_ref[:, cols]
            ).astype(jnp.bfloat16)


def attention(position, queries, kv2, kv1, kv0, gate_row, side):
    rows = queries.shape[0]
    kv_heads = kv0.shape[1] // (2 * HEAD_SIZE)
    wide = queries.shape[1] // (2 * kv_heads)
    group = wide // HEAD_SIZE
    width = kv_heads * wide
    block = math.gcd(rows, 256)
    key_spec = pl.BlockSpec((rows, HEAD_SIZE), lambda h, pos: (0, h))
    value_spec = pl.BlockSpec((rows, HEAD_SIZE), lambda h, pos: (0, kv_heads + h))
    query_spec = pl.BlockSpec((rows, wide), lambda h, pos: (0, side * kv_heads + h))
    out_spec = pl.BlockSpec((rows, wide), lambda h, pos: (0, h))
    return pl.pallas_call(
        functools.partial(attention_kernel, block=block, group=group),
        grid_spec=pltpu.PrefetchScalarGridSpec(
            num_scalar_prefetch=1,
            grid=(kv_heads,),
            in_specs=[query_spec, key_spec, key_spec, key_spec, value_spec, value_spec, value_spec,
                      pl.BlockSpec((1, wide), lambda h, pos: (0, side * kv_heads + h))],
            out_specs=[out_spec, out_spec],
        ),
        out_shape=[jax.ShapeDtypeStruct((rows, width), jnp.bfloat16)] * 2,
        compiler_params=pltpu.CompilerParams(dimension_semantics=("arbitrary",)),
        cost_estimate=pl.CostEstimate(
            flops=8 * rows * (WINDOW_TOKENS + block) * width, bytes_accessed=10 * rows * width,
            transcendentals=rows * (WINDOW_TOKENS + block) * width // HEAD_SIZE),
        name="attention",
    )(position, queries, kv2, kv1, kv0, kv2, kv1, kv0, gate_row)


def lead_kernel(tab_ref, cot_ref, away_ref, home_ref, held, *, steps, wide):
    index = pl.program_id(0)
    start = pl.multiple_of(tab_ref[index], 128)
    shift_rows = pl.multiple_of(tab_ref[steps + index], 16)
    held[...] = cot_ref[:, pl.ds(start, wide)].T
    block = held[pl.ds(shift_rows, away_ref.shape[1])]

    @pl.when(index < steps // 2)
    def _():
        away_ref[0] = block

    @pl.when(index >= steps // 2)
    def _():
        home_ref[0] = block


def lead_blocks(parity, cotangent, count):
    rows, model_width = cotangent.shape
    width = model_width // count
    wide = window_of(width)
    half = count // 2
    number = jnp.arange(half, dtype=jnp.int32) * 2
    owners = jnp.concatenate([number + 1 - parity, number + parity])
    starts = window_start(model_width, width, owners)
    table = jnp.concatenate([starts, owners * width - starts]).astype(jnp.int32)
    return pl.pallas_call(
        functools.partial(lead_kernel, steps=count, wide=wide),
        grid_spec=pltpu.PrefetchScalarGridSpec(
            num_scalar_prefetch=1,
            grid=(count,),
            in_specs=[pl.BlockSpec((rows, model_width), lambda j, tab: (0, 0))],
            out_specs=[
                pl.BlockSpec((1, width, rows), lambda j, tab: (jnp.minimum(j, half - 1), 0, 0)),
                pl.BlockSpec((1, width, rows), lambda j, tab: (jnp.maximum(j - half, 0), 0, 0)),
            ],
            scratch_shapes=[pltpu.VMEM((wide, rows), cotangent.dtype)],
        ),
        out_shape=[jax.ShapeDtypeStruct((half, width, rows), cotangent.dtype)] * 2,
        compiler_params=pltpu.CompilerParams(dimension_semantics=("arbitrary",)),
        cost_estimate=pl.CostEstimate(
            flops=8 * rows * model_width, bytes_accessed=4 * rows * model_width, transcendentals=0),
        name="lead",
    )(table, cotangent)


def terms_kernel(tab_ref, cot0_ref, cot1_ref, att0_ref, att1_ref, *out_refs, steps):
    index = pl.program_id(0)
    total = (
        jnp.dot(cot0_ref[0], att0_ref[...], preferred_element_type=jnp.float32)
        + jnp.dot(cot1_ref[0], att1_ref[...], preferred_element_type=jnp.float32)
    ).astype(jnp.bfloat16)
    sides = len(out_refs) // 2
    part = total.shape[1] // sides
    for side in range(sides):
        piece = total[:, side * part:(side + 1) * part]
        leaves = tab_ref[(1 + 3 * side) * steps + index]

        @pl.when(leaves == 1)
        def _():
            out_refs[2 * side][0] = piece

        @pl.when(leaves == 0)
        def _():
            out_refs[2 * side + 1][0] = piece


def grad_terms(position, cot_blocks, cot_other, att, att_other, order, first_bits):
    _, width, rows = cot_blocks.shape
    cols = att.shape[1]
    steps = len(order)
    sent = steps // 2
    owners = position ^ jnp.array(order, jnp.int32)
    rest = []
    for bit in first_bits:
        leaves = [1 if r & bit else 0 for r in order]
        rest += leaves
        rest += [max(sum(leaves[:j + 1]) - 1, 0) for j in range(steps)]
        rest += [max(j - sum(leaves[:j + 1]), 0) for j in range(steps)]
    sides = len(first_bits)
    table = jnp.concatenate([owners // 2, jnp.array(rest, jnp.int32)])
    whole = pl.BlockSpec((rows, cols), lambda j, tab: (0, 0))

    def out(row):
        return pl.BlockSpec((1, width, cols // sides), lambda j, tab: (tab[row * steps + j], 0, 0))

    return pl.pallas_call(
        functools.partial(terms_kernel, steps=steps),
        grid_spec=pltpu.PrefetchScalarGridSpec(
            num_scalar_prefetch=1,
            grid=(steps,),
            in_specs=[
                pl.BlockSpec((1, width, rows), lambda j, tab: (tab[j], 0, 0)),
                pl.BlockSpec((1, width, rows), lambda j, tab: (tab[j], 0, 0)),
                whole,
                whole,
            ],
            out_specs=[out(2 + 3 * (k // 2) + k % 2) for k in range(2 * sides)],
        ),
        out_shape=[jax.ShapeDtypeStruct((sent, width, cols // sides), jnp.bfloat16)]
        * (2 * sides),
        compiler_params=pltpu.CompilerParams(dimension_semantics=("arbitrary",)),
        cost_estimate=pl.CostEstimate(
            flops=4 * steps * width * rows * cols,
            bytes_accessed=2 * steps * width * (2 * rows + cols), transcendentals=0),
        name="grad_terms",
    )(table, cot_blocks, cot_other, att, att_other)


def project_kernel(pos_ref, *refs, turns, slots, count, final):
    pairs = 2 * len(turns)
    x_refs = refs[:pairs]
    rest = list(refs[pairs:])
    base_ref = rest.pop(0) if turns[0] != -1 else None
    own_ref = rest.pop(0) if turns[0] == -1 else None
    w_refs = rest[:len(slots)]
    out_ref, weight, sems = rest[len(slots):]
    position = pos_ref[0]
    copies = []
    for k, turn in enumerate(turns):
        group = []
        if turn == -1:
            start = pl.multiple_of(pos_ref[1], 128)
            group.append(pltpu.make_async_copy(
                own_ref.at[:, pl.ds(start, weight.shape[2])], weight.at[k], sems.at[k, 0]))
        else:
            for index, relative in enumerate(slots):
                start = pl.multiple_of((position ^ relative) * count, count)
                group.append(pltpu.make_async_copy(
                    w_refs[index].at[turn], weight.at[k, pl.ds(start, count)], sems.at[k, index]))
        for copy in group:
            copy.start()
        copies.append(group)
    total = None if base_ref is None else base_ref[...]
    middle = x_refs[0].shape[1]
    for k in range(len(turns)):
        for copy in copies[k]:
            copy.wait()
        for side in range(2):
            part = jnp.dot(
                x_refs[2 * k + side][...],
                weight[k, side * middle:(side + 1) * middle],
                preferred_element_type=jnp.float32,
            )
            total = part if total is None else total + part
    if final:
        wide = total.shape[1]
        total = pltpu.roll(total, lax.rem(wide - pos_ref[2], wide), 1)[:, :out_ref.shape[1]]
    out_ref[...] = total.astype(out_ref.dtype)


def project(position, xs, base, own, weights, slots, turns, out_cols, dtype):
    rows, middle = xs[0].shape
    cols = weights[0].shape[2]
    whole = pl.BlockSpec(memory_space=pltpu.VMEM)
    anywhere = pl.BlockSpec(memory_space=pl.ANY)
    extra = [own] if base is None else [base]
    return pl.pallas_call(
        functools.partial(project_kernel, turns=turns, slots=slots, count=2 * middle // len(slots),
                          final=base is not None),
        in_specs=[pl.BlockSpec(memory_space=pltpu.SMEM)] + [whole] * len(xs)
        + [anywhere if base is None else whole] + [anywhere] * len(weights),
        out_specs=whole,
        out_shape=jax.ShapeDtypeStruct((rows, out_cols), dtype),
        scratch_shapes=[
            pltpu.VMEM((len(turns), 2 * middle, cols), jnp.bfloat16),
            pltpu.SemaphoreType.DMA((len(turns), len(slots))),
        ],
        cost_estimate=pl.CostEstimate(
            flops=4 * len(turns) * rows * middle * cols,
            bytes_accessed=len(turns) * 4 * middle * (rows + cols) + 8 * rows * cols,
            transcendentals=0),
        name="project",
    )(position, *xs, *extra, *weights)


def finish_kernel(*refs, counts):
    w_ref, gate_ref, grad_ref, product_ref = refs[-4:]
    place = 0
    for side, count in enumerate(counts):
        total = refs[place][0].astype(jnp.float32)
        for ref in refs[place + 1:place + count]:
            total = total + ref[0].astype(jnp.float32)
        place += count
        cols = slice(side * total.shape[1], (side + 1) * total.shape[1])
        grad_ref[:, cols] = total * gate_ref[:, cols]
        weighted = total * w_ref[:total.shape[0], cols].astype(jnp.float32)
        product_ref[:, cols] = jnp.sum(weighted, axis=0, keepdims=True)


def finish(grads, w_mine, scale_row):
    in_specs = []
    operands = []
    for terms in grads:
        for array, index in terms:
            in_specs.append(
                pl.BlockSpec((1,) + array.shape[1:], functools.partial(first_at, index)))
            operands.append(array)
    width = grads[0][0][0].shape[1]
    depth = w_mine.shape[1]
    whole = [w_mine.shape, (1, depth)]
    return pl.pallas_call(
        functools.partial(finish_kernel, counts=tuple(len(terms) for terms in grads)),
        grid=(1,),
        in_specs=in_specs + [pl.BlockSpec(shape, lambda g: (0, 0)) for shape in whole],
        out_specs=[pl.BlockSpec((width, depth), lambda g: (0, 0)),
                   pl.BlockSpec((1, depth), lambda g: (0, 0))],
        out_shape=[jax.ShapeDtypeStruct((width, depth), jnp.float32),
                   jax.ShapeDtypeStruct((1, depth), jnp.float32)],
        cost_estimate=pl.CostEstimate(
            flops=8 * width * depth, bytes_accessed=12 * width * depth, transcendentals=0),
        name="finish",
    )(*operands, w_mine, scale_row)


def first_at(index, step):
    return (index, 0, 0)


def turned_kernel(pos_ref, w_ref, out_ref, held, flipped, sem):
    start = pl.multiple_of(pos_ref[3], 128)
    copy = pltpu.make_async_copy(w_ref.at[:, pl.ds(start, held.shape[1])], held, sem)
    copy.start()
    copy.wait()
    flipped[...] = held[...].T
    out_ref[...] = flipped[pl.ds(pl.multiple_of(pos_ref[4], 16), out_ref.shape[0])]


def turned(position, w_out, cols):
    wide = window_of(cols)
    return pl.pallas_call(
        turned_kernel,
        in_specs=[pl.BlockSpec(memory_space=pltpu.SMEM), pl.BlockSpec(memory_space=pl.ANY)],
        out_specs=pl.BlockSpec(memory_space=pltpu.VMEM),
        out_shape=jax.ShapeDtypeStruct((cols, w_out.shape[0]), w_out.dtype),
        scratch_shapes=[pltpu.VMEM((w_out.shape[0], wide), w_out.dtype),
                        pltpu.VMEM((wide, w_out.shape[0]), w_out.dtype),
                        pltpu.SemaphoreType.DMA],
        name="turned",
    )(position, w_out)


def body(tokens, norm_gain, w_query, w_key, value_weight, w_out, mask_logit, noise_draw, cotangent):
    tok_rows, model_width = tokens.shape
    local_heads = mask_logit.shape[0]
    n_ctx = lax.axis_size("ctx")
    n_head = lax.axis_size("head")
    p = lax.axis_index("ctx")
    z = lax.axis_index("head")
    bits = [1 << k for k in range(1, n_ctx.bit_length() - 1)]
    inv_root = 1.0 / math.sqrt(tok_rows * n_ctx)
    out_cols = model_width // n_head
    own_cols = model_width // n_ctx
    wide_cols = window_of(out_cols)
    own_start = window_start(model_width, out_cols, z)
    mine_start = window_start(model_width, own_cols, p)
    scalars = jnp.stack(
        [p, own_start, z * out_cols - own_start, mine_start, p * own_cols - mine_start]).astype(jnp.int32)
    position = scalars[:1]
    piece = w_out.shape[0] // n_ctx

    mine = lax.dynamic_slice_in_dim(w_out, p * piece, piece, 0)
    turns = []
    for t in range(1, n_head):
        block = lax.dynamic_slice_in_dim(
            mine, window_start(model_width, out_cols, (z + t) % n_head), wide_cols, 1)
        turns.append(rotate(block, "head", t))

    widened = tokens.astype(jnp.float32)
    moment = jnp.mean(jnp.square(widened), axis=1, keepdims=True)
    normed = (
        widened * lax.rsqrt(moment + EPSILON) * norm_gain.astype(jnp.float32)[None, :]
    ).astype(jnp.bfloat16)
    keys = jnp.dot(normed, w_key, preferred_element_type=jnp.float32).astype(jnp.bfloat16)
    values = jnp.dot(normed, value_weight, preferred_element_type=jnp.float32).astype(
        jnp.bfloat16)
    kv_half = keys.shape[1] // 2
    kv_sides = []
    kv2_sides = []
    for h in range(2):
        cols = slice(h * kv_half, (h + 1) * kv_half)
        kv_sides.append(jnp.concatenate([keys[:, cols], values[:, cols]], axis=1))
        kv2_sides.append(shift(kv_sides[h], "ctx", 2))
    queries = jnp.dot(
        after(normed, *kv_sides), w_query, preferred_element_type=jnp.float32
    ).astype(jnp.bfloat16)

    gate_value, gate_slope, penalty_term = hard_concrete(mask_logit, noise_draw)
    gate_columns = jnp.repeat(gate_value, HEAD_SIZE)
    gate_row = gate_columns[None, :]

    own_part = jnp.stack(after(tuple(turns), queries))
    parts = {0: own_part}
    for bit in bits:
        for relative in list(parts):
            parts[relative | bit] = swap(parts[relative], "ctx", bit)

    mixed = [jnp.where(p % 2 == 0, kv_sides[h], after(kv2_sides[h], queries)) for h in range(2)]

    attended = []
    moving = []
    others = []
    for h in range(2):
        kv1 = swap(mixed[h], "ctx", 1)
        att, gat = attention(
            position, queries, kv2_sides[h], kv1, kv_sides[h], gate_row, h)
        attended.append(att)
        chain = [gat]
        for _ in range(1, n_head):
            chain.append(rotate(chain[-1], "head", 1))
        moving.append(chain)
        others.append(swap(att, "ctx", 1))
        if h == 0:
            leaving, cot_home = lead_blocks(after(p % 2, att), cotangent, n_ctx)
            cot_other = swap(leaving, "ctx", 1)

    w_mine = turned(after(scalars, attended[1]), w_out, own_cols)

    grads = []
    relative = [2 * j for j in range(n_ctx // 2)]
    for h in range(2):
        orders = (bits, bits[::-1])
        blocks = grad_terms(
            position, cot_home, cot_other, attended[h], others[h], relative[::-1],
            [order[0] for order in orders])
        for side, order in enumerate(orders):
            sent, kept = blocks[2 * side:2 * side + 2]
            left = [r for r in relative[::-1] if not r & order[0]]
            held = [[(kept, i)] for i in range(len(left))]
            for k, bit in enumerate(order):
                if k:
                    leave = [i for i, r in enumerate(left) if r & bit]
                    stay = [i for i, r in enumerate(left) if not r & bit]
                    sent = jnp.concatenate(
                        [sum(a[i:i + 1].astype(jnp.float32) for a, i in held[index])
                         for index in leave], axis=0).astype(jnp.bfloat16)
                    held = [held[i] for i in stay]
                    left = [left[i] for i in stay]
                received = swap(sent, "ctx", bit)
                held = [terms + [(received, i)] for i, terms in enumerate(held)]
            grads.append(held[0])

    for relative in list(parts):
        parts[relative | 1] = swap(parts[relative], "ctx", 1)
    slots = tuple(parts)
    weights = [parts[r] for r in slots]

    early = list(range(n_head - 2))
    xs = [moving[h][0] for h in range(2)]
    for t in early:
        xs += [moving[h][t + 1] for h in range(2)]
    base = project(scalars, xs, None, w_out, weights, slots, (-1,) + tuple(early),
                   wide_cols, jnp.float32)
    layer_out = project(scalars, [moving[h][-1] for h in range(2)], base, None, weights,
                        slots, (n_head - 2,), out_cols, jnp.bfloat16)

    grad_columns, products = finish(grads, w_mine, gate_row * inv_root)
    grad_out_proj = grad_columns.T
    head_terms = jnp.sum(products.reshape(local_heads, HEAD_SIZE), axis=1)
    values = [head_terms]
    for member in range(1, n_ctx):
        values.append(swap(head_terms, "ctx", member))
    while len(values) > 1:
        values = [values[i] + values[i + 1] for i in range(0, len(values), 2)]
    grad_logit = values[0] * inv_root * gate_slope + penalty_term
    return (layer_out, grad_logit, grad_out_proj)


def solution(mesh):
    return jax.shard_map(
        body,
        mesh=mesh,
        in_specs=(
            P("ctx", None),
            P(),
            P(None, "head"),
            P(None, "head"),
            P(None, "head"),
            P("head", None),
            P("head"),
            P("head"),
            P("ctx", None),
        ),
        out_specs=(P("ctx", "head"), P("head"), P("head", "ctx")),
        check_vma=False,
    )
```

```python
import functools
import math

import jax
import jax.numpy as jnp
from jax import lax
from jax.experimental import pallas as pl
from jax.experimental.pallas import tpu as pltpu
from jax.sharding import PartitionSpec as P


HEAD_SIZE = 128
WINDOW_TOKENS = 1024

EPSILON = 1e-06
BETA = 2.0 / 3.0
GAMMA = -0.1
ZETA = 1.1
PENALTY = 0.1
SCORE_SCALE = 168.0 ** (-0.5)
LOG2_E = 1.4426950408889634


def shift(value, axis, steps):
    count = lax.axis_size(axis)
    return lax.ppermute(value, axis, [(i, i + steps) for i in range(count - steps)])


def rotate(value, axis, steps):
    count = lax.axis_size(axis)
    return lax.ppermute(value, axis, [(i, (i + steps) % count) for i in range(count)])


def swap(value, axis, bit):
    count = lax.axis_size(axis)
    return lax.ppermute(value, axis, [(i, i ^ bit) for i in range(count)])


def window_of(cols):
    step = math.gcd(cols, 128)
    return -(-(cols + 128 - step) // 128) * 128


def window_start(width, cols, index):
    first = index * cols // 128 * 128
    return jnp.minimum(first, width - window_of(cols))


def hard_concrete(mask_logit, noise_draw):
    stretched = jax.nn.sigmoid(
        (jnp.log(noise_draw) - jnp.log(1.0 - noise_draw) + mask_logit) / BETA
    )
    shifted = stretched * (ZETA - GAMMA) + GAMMA
    gate_value = jnp.clip(shifted, 0.0, 1.0)
    inside = jnp.logical_and(shifted > 0.0, shifted < 1.0)
    gate_slope = jnp.where(inside, (ZETA - GAMMA) * stretched * (1.0 - stretched) / BETA, 0.0)
    expected = jax.nn.sigmoid(mask_logit - BETA * math.log(-GAMMA / ZETA))
    return (gate_value, gate_slope, PENALTY * expected * (1.0 - expected))


def after(value, *others):
    return lax.optimization_barrier((value,) + others)[0]


def attention_kernel(pos_ref, q_ref, k2_ref, k1_ref, k0_ref, v2_ref, v1_ref, v0_ref, gate_ref,
                     att_ref, gated_ref, *, block, group):
    rows = q_ref.shape[0]
    position = pos_ref[0]
    keys = (k2_ref, k1_ref, k0_ref)
    values = (v2_ref, v1_ref, v0_ref)
    bias = (
        jnp.where(position >= 2, 0.0, -jnp.inf).astype(jnp.float32),
        jnp.where(position >= 1, 0.0, -jnp.inf).astype(jnp.float32),
        None,
    )
    per = rows // block
    count = WINDOW_TOKENS // block + 1
    ones = jnp.ones((block, HEAD_SIZE), jnp.bfloat16)
    row_id = lax.broadcasted_iota(jnp.int32, (block, block), 0)
    col_id = lax.broadcasted_iota(jnp.int32, (block, block), 1)
    behind = jnp.concatenate([col_id > row_id] * group, axis=0)
    ahead = jnp.concatenate([col_id <= row_id] * group, axis=0)
    for b in range(per):
        here = pl.ds(b * block, block)
        query = jnp.concatenate(
            [q_ref[here, g * HEAD_SIZE:(g + 1) * HEAD_SIZE] for g in range(group)], axis=0
        )
        scores = []
        for s in range(count):
            piece, offset = divmod(b + s, per)
            key = keys[piece][pl.ds(offset * block, block), :]
            score = lax.dot_general(
                query, key, (((1,), (1,)), ((), ())), preferred_element_type=jnp.float32
            )
            if s == 0:
                score = jnp.where(behind, score, -jnp.inf)
            if s == count - 1:
                score = jnp.where(ahead, score, -jnp.inf)
            if bias[piece] is not None:
                score = score + bias[piece]
            scores.append(score)
        top = functools.reduce(jnp.maximum, scores)
        top = jnp.max(top, axis=1, keepdims=True)
        total = None
        for s in range(count):
            piece, offset = divmod(b + s, per)
            prob = jnp.exp2((scores[s] - top) * (SCORE_SCALE * LOG2_E)).astype(jnp.bfloat16)
            value = jnp.concatenate(
                [values[piece][pl.ds(offset * block, block), :], ones], axis=1
            )
            part = jnp.dot(prob, value, preferred_element_type=jnp.float32)
            total = part if total is None else total + part
        result = (total[:, :HEAD_SIZE] / total[:, HEAD_SIZE:]).astype(jnp.bfloat16)
        for g in range(group):
            cols = slice(g * HEAD_SIZE, (g + 1) * HEAD_SIZE)
            piece_out = result[g * block:(g + 1) * block]
            att_ref[here, cols] = piece_out
            gated_ref[here, cols] = (
                piece_out.astype(jnp.float32) * gate_ref[:, cols]
            ).astype(jnp.bfloat16)


def attention(position, queries, kv2, kv1, kv0, gate_row, side):
    rows = queries.shape[0]
    all_heads = kv0.shape[1] // (2 * HEAD_SIZE)
    kv_heads = all_heads // 2
    wide = queries.shape[1] // (2 * kv_heads)
    group = wide // HEAD_SIZE
    width = kv_heads * wide
    block = math.gcd(rows, 256)
    key_spec = pl.BlockSpec((rows, HEAD_SIZE), lambda h, pos: (0, side * kv_heads + h))
    value_spec = pl.BlockSpec((rows, HEAD_SIZE), lambda h, pos: (0, all_heads + side * kv_heads + h))
    query_spec = pl.BlockSpec((rows, wide), lambda h, pos: (0, side * kv_heads + h))
    out_spec = pl.BlockSpec((rows, wide), lambda h, pos: (0, h))
    return pl.pallas_call(
        functools.partial(attention_kernel, block=block, group=group),
        grid_spec=pltpu.PrefetchScalarGridSpec(
            num_scalar_prefetch=1,
            grid=(kv_heads,),
            in_specs=[query_spec, key_spec, key_spec, key_spec, value_spec, value_spec, value_spec,
                      pl.BlockSpec((1, wide), lambda h, pos: (0, side * kv_heads + h))],
            out_specs=[out_spec, out_spec],
        ),
        out_shape=[jax.ShapeDtypeStruct((rows, width), jnp.bfloat16)] * 2,
        compiler_params=pltpu.CompilerParams(dimension_semantics=("arbitrary",)),
        cost_estimate=pl.CostEstimate(
            flops=8 * rows * (WINDOW_TOKENS + block) * width, bytes_accessed=10 * rows * width,
            transcendentals=rows * (WINDOW_TOKENS + block) * width // HEAD_SIZE),
        name="attention",
    )(position, queries, kv2, kv1, kv0, kv2, kv1, kv0, gate_row)


def lead_kernel(tab_ref, cot_ref, away_ref, home_ref, held, *, steps, wide):
    index = pl.program_id(0)
    start = pl.multiple_of(tab_ref[index], 128)
    shift_rows = pl.multiple_of(tab_ref[steps + index], 16)
    held[...] = cot_ref[:, pl.ds(start, wide)].T
    block = held[pl.ds(shift_rows, away_ref.shape[1])]

    @pl.when(index < steps // 2)
    def _():
        away_ref[0] = block

    @pl.when(index >= steps // 2)
    def _():
        home_ref[0] = block


def lead_blocks(parity, cotangent, count):
    rows, model_width = cotangent.shape
    width = model_width // count
    wide = window_of(width)
    half = count // 2
    number = jnp.arange(half, dtype=jnp.int32) * 2
    owners = jnp.concatenate([number + 1 - parity, number + parity])
    starts = window_start(model_width, width, owners)
    table = jnp.concatenate([starts, owners * width - starts]).astype(jnp.int32)
    return pl.pallas_call(
        functools.partial(lead_kernel, steps=count, wide=wide),
        grid_spec=pltpu.PrefetchScalarGridSpec(
            num_scalar_prefetch=1,
            grid=(count,),
            in_specs=[pl.BlockSpec((rows, model_width), lambda j, tab: (0, 0))],
            out_specs=[
                pl.BlockSpec((1, width, rows), lambda j, tab: (jnp.minimum(j, half - 1), 0, 0)),
                pl.BlockSpec((1, width, rows), lambda j, tab: (jnp.maximum(j - half, 0), 0, 0)),
            ],
            scratch_shapes=[pltpu.VMEM((wide, rows), cotangent.dtype)],
        ),
        out_shape=[jax.ShapeDtypeStruct((half, width, rows), cotangent.dtype)] * 2,
        compiler_params=pltpu.CompilerParams(dimension_semantics=("arbitrary",)),
        cost_estimate=pl.CostEstimate(
            flops=8 * rows * model_width, bytes_accessed=4 * rows * model_width, transcendentals=0),
        name="lead",
    )(table, cotangent)


def terms_kernel(tab_ref, cot0_ref, cot1_ref, att0_ref, att1_ref, *out_refs, steps):
    index = pl.program_id(0)
    total = (
        jnp.dot(cot0_ref[0], att0_ref[...], preferred_element_type=jnp.float32)
        + jnp.dot(cot1_ref[0], att1_ref[...], preferred_element_type=jnp.float32)
    ).astype(jnp.bfloat16)
    sides = len(out_refs) // 2
    part = total.shape[1] // sides
    for side in range(sides):
        piece = total[:, side * part:(side + 1) * part]
        leaves = tab_ref[(1 + 3 * side) * steps + index]

        @pl.when(leaves == 1)
        def _():
            out_refs[2 * side][0] = piece

        @pl.when(leaves == 0)
        def _():
            out_refs[2 * side + 1][0] = piece


def grad_terms(position, cot_blocks, cot_other, att, att_other, order, first_bits):
    _, width, rows = cot_blocks.shape
    cols = att.shape[1]
    steps = len(order)
    sent = steps // 2
    owners = position ^ jnp.array(order, jnp.int32)
    rest = []
    for bit in first_bits:
        leaves = [1 if r & bit else 0 for r in order]
        rest += leaves
        rest += [max(sum(leaves[:j + 1]) - 1, 0) for j in range(steps)]
        rest += [max(j - sum(leaves[:j + 1]), 0) for j in range(steps)]
    sides = len(first_bits)
    table = jnp.concatenate([owners // 2, jnp.array(rest, jnp.int32)])
    whole = pl.BlockSpec((rows, cols), lambda j, tab: (0, 0))

    def out(row):
        return pl.BlockSpec((1, width, cols // sides), lambda j, tab: (tab[row * steps + j], 0, 0))

    return pl.pallas_call(
        functools.partial(terms_kernel, steps=steps),
        grid_spec=pltpu.PrefetchScalarGridSpec(
            num_scalar_prefetch=1,
            grid=(steps,),
            in_specs=[
                pl.BlockSpec((1, width, rows), lambda j, tab: (tab[j], 0, 0)),
                pl.BlockSpec((1, width, rows), lambda j, tab: (tab[j], 0, 0)),
                whole,
                whole,
            ],
            out_specs=[out(2 + 3 * (k // 2) + k % 2) for k in range(2 * sides)],
        ),
        out_shape=[jax.ShapeDtypeStruct((sent, width, cols // sides), jnp.bfloat16)]
        * (2 * sides),
        compiler_params=pltpu.CompilerParams(dimension_semantics=("arbitrary",)),
        cost_estimate=pl.CostEstimate(
            flops=4 * steps * width * rows * cols,
            bytes_accessed=2 * steps * width * (2 * rows + cols), transcendentals=0),
        name="grad_terms",
    )(table, cot_blocks, cot_other, att, att_other)


def project_kernel(pos_ref, *refs, turns, slots, count, final):
    pairs = 2 * len(turns)
    x_refs = refs[:pairs]
    rest = list(refs[pairs:])
    base_ref = rest.pop(0) if turns[0] != -1 else None
    own_ref = rest.pop(0) if turns[0] == -1 else None
    w_refs = rest[:len(slots)]
    out_ref, weight, flipped, sems = rest[len(slots):]
    position = pos_ref[0]
    copies = []
    for k, turn in enumerate(turns):
        group = []
        if turn == -1:
            start = pl.multiple_of(pos_ref[1], 128)
            group.append(pltpu.make_async_copy(
                own_ref.at[:, pl.ds(start, weight.shape[2])], weight.at[k], sems.at[k, 0]))
        else:
            for index, relative in enumerate(slots):
                start = pl.multiple_of((position ^ relative) * count, count)
                group.append(pltpu.make_async_copy(
                    w_refs[index].at[turn], weight.at[k, pl.ds(start, count)], sems.at[k, index]))
        for copy in group:
            copy.start()
        copies.append(group)
    total = None if base_ref is None else base_ref[...]
    middle = x_refs[0].shape[1]
    for k in range(len(turns)):
        for copy in copies[k]:
            copy.wait()
        for side in range(2):
            part = jnp.dot(
                x_refs[2 * k + side][...],
                weight[k, side * middle:(side + 1) * middle],
                preferred_element_type=jnp.float32,
            )
            total = part if total is None else total + part
    if final:
        flipped[...] = total.astype(flipped.dtype).T
        out_ref[...] = flipped[pl.ds(pl.multiple_of(pos_ref[2], 16), out_ref.shape[0])]
    else:
        out_ref[...] = total


def project(position, xs, base, own, weights, slots, turns, out_cols, dtype):
    rows, middle = xs[0].shape
    cols = weights[0].shape[2]
    whole = pl.BlockSpec(memory_space=pltpu.VMEM)
    anywhere = pl.BlockSpec(memory_space=pl.ANY)
    extra = [own] if base is None else [base]
    return pl.pallas_call(
        functools.partial(project_kernel, turns=turns, slots=slots, count=2 * middle // len(slots),
                          final=base is not None),
        in_specs=[pl.BlockSpec(memory_space=pltpu.SMEM)] + [whole] * len(xs)
        + [anywhere if base is None else whole] + [anywhere] * len(weights),
        out_specs=whole,
        out_shape=jax.ShapeDtypeStruct(
            (rows, out_cols) if base is None else (out_cols, rows), dtype),
        scratch_shapes=[
            pltpu.VMEM((len(turns), 2 * middle, cols), jnp.bfloat16),
            pltpu.VMEM((cols, rows) if base is not None else (16, 128), jnp.bfloat16),
            pltpu.SemaphoreType.DMA((len(turns), len(slots))),
        ],
        cost_estimate=pl.CostEstimate(
            flops=4 * len(turns) * rows * middle * cols,
            bytes_accessed=len(turns) * 4 * middle * (rows + cols) + 8 * rows * cols,
            transcendentals=0),
        name="project",
    )(position, *xs, *extra, *weights)


def finish_kernel(*refs, counts):
    w_ref, gate_ref, grad_ref, product_ref = refs[-4:]
    place = 0
    for side, count in enumerate(counts):
        total = refs[place][0].astype(jnp.float32)
        for ref in refs[place + 1:place + count]:
            total = total + ref[0].astype(jnp.float32)
        place += count
        cols = slice(side * total.shape[1], (side + 1) * total.shape[1])
        grad_ref[:, cols] = total * gate_ref[:, cols]
        weighted = total * w_ref[:total.shape[0], cols].astype(jnp.float32)
        product_ref[:, cols] = jnp.sum(weighted, axis=0, keepdims=True)


def finish(grads, w_mine, scale_row):
    in_specs = []
    operands = []
    for terms in grads:
        for array, index in terms:
            in_specs.append(
                pl.BlockSpec((1,) + array.shape[1:], functools.partial(first_at, index)))
            operands.append(array)
    width = grads[0][0][0].shape[1]
    depth = w_mine.shape[1]
    whole = [w_mine.shape, (1, depth)]
    return pl.pallas_call(
        functools.partial(finish_kernel, counts=tuple(len(terms) for terms in grads)),
        grid=(1,),
        in_specs=in_specs + [pl.BlockSpec(shape, lambda g: (0, 0)) for shape in whole],
        out_specs=[pl.BlockSpec((width, depth), lambda g: (0, 0)),
                   pl.BlockSpec((1, depth), lambda g: (0, 0))],
        out_shape=[jax.ShapeDtypeStruct((width, depth), jnp.float32),
                   jax.ShapeDtypeStruct((1, depth), jnp.float32)],
        cost_estimate=pl.CostEstimate(
            flops=8 * width * depth, bytes_accessed=12 * width * depth, transcendentals=0),
        name="finish",
    )(*operands, w_mine, scale_row)


def first_at(index, step):
    return (index, 0, 0)


def turned_kernel(pos_ref, w_ref, out_ref, held, flipped, sem):
    start = pl.multiple_of(pos_ref[3], 128)
    copy = pltpu.make_async_copy(w_ref.at[:, pl.ds(start, held.shape[1])], held, sem)
    copy.start()
    copy.wait()
    flipped[...] = held[...].T
    out_ref[...] = flipped[pl.ds(pl.multiple_of(pos_ref[4], 16), out_ref.shape[0])]


def turned(position, w_out, cols):
    wide = window_of(cols)
    return pl.pallas_call(
        turned_kernel,
        in_specs=[pl.BlockSpec(memory_space=pltpu.SMEM), pl.BlockSpec(memory_space=pl.ANY)],
        out_specs=pl.BlockSpec(memory_space=pltpu.VMEM),
        out_shape=jax.ShapeDtypeStruct((cols, w_out.shape[0]), w_out.dtype),
        scratch_shapes=[pltpu.VMEM((w_out.shape[0], wide), w_out.dtype),
                        pltpu.VMEM((wide, w_out.shape[0]), w_out.dtype),
                        pltpu.SemaphoreType.DMA],
        name="turned",
    )(position, w_out)


def body(tokens, norm_gain, w_query, w_key, value_weight, w_out, mask_logit, noise_draw, cotangent):
    tok_rows, model_width = tokens.shape
    local_heads = mask_logit.shape[0]
    n_ctx = lax.axis_size("ctx")
    n_head = lax.axis_size("head")
    p = lax.axis_index("ctx")
    z = lax.axis_index("head")
    bits = [1 << k for k in range(1, n_ctx.bit_length() - 1)]
    inv_root = 1.0 / math.sqrt(tok_rows * n_ctx)
    out_cols = model_width // n_head
    own_cols = model_width // n_ctx
    wide_cols = window_of(out_cols)
    own_start = window_start(model_width, out_cols, z)
    mine_start = window_start(model_width, own_cols, p)
    scalars = jnp.stack(
        [p, own_start, z * out_cols - own_start, mine_start, p * own_cols - mine_start]).astype(jnp.int32)
    position = scalars[:1]
    piece = w_out.shape[0] // n_ctx

    mine = lax.dynamic_slice_in_dim(w_out, p * piece, piece, 0)
    turns = []
    for t in range(1, n_head):
        block = lax.dynamic_slice_in_dim(
            mine, window_start(model_width, out_cols, (z + t) % n_head), wide_cols, 1)
        turns.append(rotate(block, "head", t))

    widened = tokens.astype(jnp.float32)
    moment = jnp.mean(jnp.square(widened), axis=1, keepdims=True)
    normed = (
        widened * lax.rsqrt(moment + EPSILON) * norm_gain.astype(jnp.float32)[None, :]
    ).astype(jnp.bfloat16)
    keys = jnp.dot(normed, w_key, preferred_element_type=jnp.float32).astype(jnp.bfloat16)
    values = jnp.dot(normed, value_weight, preferred_element_type=jnp.float32).astype(
        jnp.bfloat16)
    kv0 = jnp.concatenate([keys, values], axis=1)
    kv2 = shift(kv0, "ctx", 2)
    queries = jnp.dot(
        after(normed, kv0), w_query, preferred_element_type=jnp.float32
    ).astype(jnp.bfloat16)

    gate_value, gate_slope, penalty_term = hard_concrete(mask_logit, noise_draw)
    gate_columns = jnp.repeat(gate_value, HEAD_SIZE)
    gate_row = gate_columns[None, :]

    own_part = jnp.stack(after(tuple(turns), queries))
    parts = {0: own_part}
    for bit in bits:
        for relative in list(parts):
            parts[relative | bit] = swap(parts[relative], "ctx", bit)

    leaving, cot_home = lead_blocks(after(p % 2, own_part), cotangent, n_ctx)
    cot_other = swap(leaving, "ctx", 1)
    mixed = jnp.where(p % 2 == 0, kv0, after(kv2, cot_home))
    kv1 = swap(mixed, "ctx", 1)
    w_mine = turned(after(scalars, mixed), w_out, own_cols)

    attended = []
    moving = []
    others = []
    for h in range(2):
        att, gat = attention(
            position, queries, kv2, kv1, kv0, gate_row, h)
        attended.append(att)
        chain = [gat]
        for _ in range(1, n_head):
            chain.append(rotate(chain[-1], "head", 1))
        moving.append(chain)
        others.append(swap(att, "ctx", 1))


    grads = []
    relative = [2 * j for j in range(n_ctx // 2)]
    for h in range(2):
        orders = (bits, bits[::-1])
        blocks = grad_terms(
            position, cot_home, cot_other, attended[h], others[h], relative[::-1],
            [order[0] for order in orders])
        for side, order in enumerate(orders):
            sent, kept = blocks[2 * side:2 * side + 2]
            left = [r for r in relative[::-1] if not r & order[0]]
            held = [[(kept, i)] for i in range(len(left))]
            for k, bit in enumerate(order):
                if k:
                    leave = [i for i, r in enumerate(left) if r & bit]
                    stay = [i for i, r in enumerate(left) if not r & bit]
                    sent = jnp.concatenate(
                        [sum(a[i:i + 1].astype(jnp.float32) for a, i in held[index])
                         for index in leave], axis=0).astype(jnp.bfloat16)
                    held = [held[i] for i in stay]
                    left = [left[i] for i in stay]
                received = swap(sent, "ctx", bit)
                held = [terms + [(received, i)] for i, terms in enumerate(held)]
            grads.append(held[0])

    for relative in list(parts):
        parts[relative | 1] = swap(parts[relative], "ctx", 1)
    slots = tuple(parts)
    weights = [parts[r] for r in slots]

    late = tuple(range(max(n_head - 3, 0), n_head - 1))
    early = tuple(range(late[0]))
    pairs = [[moving[h][t + 1] for h in range(2)] for t in range(n_head - 1)]
    xs = [moving[h][0] for h in range(2)] + sum((pairs[t] for t in early), [])
    base = project(scalars, xs, None, w_out, weights, slots, (-1,) + early, wide_cols,
                   jnp.float32)
    layer_out = project(scalars, sum((pairs[t] for t in late), []), base, None, weights,
                        slots, late, out_cols, jnp.bfloat16).T

    grad_columns, products = finish(grads, w_mine, gate_row * inv_root)
    grad_out_proj = grad_columns.T
    head_terms = jnp.sum(products.reshape(local_heads, HEAD_SIZE), axis=1)
    for bit in [1] + bits:
        head_terms = head_terms + swap(head_terms, "ctx", bit)
    grad_logit = head_terms * inv_root * gate_slope + penalty_term
    return (layer_out, grad_logit, grad_out_proj)


def solution(mesh):
    return jax.shard_map(
        body,
        mesh=mesh,
        in_specs=(
            P("ctx", None),
            P(),
            P(None, "head"),
            P(None, "head"),
            P(None, "head"),
            P("head", None),
            P("head"),
            P("head"),
            P("ctx", None),
        ),
        out_specs=(P("ctx", "head"), P("head"), P("head", "ctx")),
        check_vma=False,
    )
```
